32 devices in a mesh: seq: 8 (over z, y), tp: 4 (over x, core).
Axes of the slice: x: 2, y: 2, z: 4, core: 2. Of those that a mesh axis runs over, the one named last changes fastest.
Arguments:
- tokens: bfloat16 [8192, 2048], P('seq', 'tp'), may hold values from -8 to 8
- col_order: int32 [8192], P('seq'), may hold values from 0 to 8191, as said below
- in_gain: float32 [2, 2048], replicated, may hold values from 0.5 to 1.5
- w_in: bfloat16 [2, 2048, 2, 2048], P(None, None, None, 'tp'), may hold values from -0.125 to 0.125
- w_bc: bfloat16 [2, 2048, 256], replicated, may hold values from -0.0625 to 0.0625
- w_dt: bfloat16 [2, 2048, 32], P(None, None, 'tp'), may hold values from -2 to 2
- conv_x: float32 [2, 4, 2048], P(None, None, 'tp'), may hold values from -3 to 3
- conv_bc: float32 [2, 4, 256], replicated, may hold values from -3 to 3
- dt_bias: float32 [2, 32], P(None, 'tp'), may hold values from -1 to 0.5
- a_log: float32 [2, 32], P(None, 'tp'), may hold values from -16 to -2, as said below
- d_skip: float32 [2, 32], P(None, 'tp'), may hold values from 0.5 to 2
- out_gain: float32 [2, 2048], P(None, 'tp'), may hold values from 0.5 to 1.5
- w_out: bfloat16 [2, 2048, 2048], P(None, 'tp'), may hold values from -0.125 to 0.125
Outputs:
- mixed_out: bfloat16 [8192, 2048], P('seq', 'tp')
The draws below stay inside these ranges and needn't reach their ends.
Inputs may be any that keep to these rules, and one draw needn't show every extreme that they name: `col_order`: A permutation of the 8192 positions of a frame of 16 rows and 512 columns stored row by row: the column order visits the columns one after another in a drawn order, each from top to bottom or from bottom to top as drawn. So every aligned block of 1024 positions takes exactly 128 row-order positions from each aligned block of 1024 row-order positions. Each head's decay rate exp(a_log) is either between about one in fifty and one in seventeen a step or between 0.3 / 8192 and 2 / 8192 a step.
All inputs are finite; a program needn't handle non-finite values.
Results may differ from the reference program's by a relative error of at most 0.024.
Values may be sent and summed in bfloat16 or wider, within the bound.
A program may use at most 128 MiB of HBM per device.

```python
import math
import jax
import jax.numpy as jnp
from jax import lax

D = 2048
HEADS = 32
HEAD_DIM = 64
STATE = 128
CONV = 4
STRETCH = 128
WIDTH_CELLS = 512
INNER = 2048
FRAME_ROWS = 16
TOKENS = 8192
N_TP = 4


def shared_direction(key):
    raw = jax.random.normal(jax.random.fold_in(key, 31), (D,), dtype=jnp.float32)
    return raw / jnp.sqrt(jnp.sum(raw * raw))


def draw_tokens(key, part):
    direction = shared_direction(key)
    noise_key, level_key = jax.random.split(jax.random.fold_in(key, 17), 2)
    noise = jnp.clip(jax.random.normal(noise_key, (TOKENS, D), dtype=jnp.float32), -6.0, 6.0)
    levels = jax.random.uniform(level_key, (FRAME_ROWS,), minval=-3.0, maxval=3.0)
    along = jnp.repeat(levels, WIDTH_CELLS, total_repeat_length=TOKENS)
    return (noise + along[:, None] * direction[None, :]).astype(jnp.bfloat16)


def draw_w_dt(key, part):
    direction = shared_direction(key)
    base_key, amp_key = jax.random.split(jax.random.fold_in(key, 19), 2)
    base = jnp.clip(jax.random.normal(base_key, (2, D, HEADS), dtype=jnp.float32), -4.0, 4.0) / math.sqrt(D)
    amplitude = jax.random.uniform(amp_key, (2, HEADS), minval=0.5, maxval=1.5)
    return (base + direction[None, :, None] * amplitude[:, None, :]).astype(jnp.bfloat16)


def draw_a_log(key, part):
    base = jax.random.fold_in(key, 7)
    pick_key, fast_key, slow_key = jax.random.split(base, 3)
    share = 0.5
    fast = jax.random.uniform(pick_key, (2, HEADS)) < share
    fast_rate = jnp.exp(jax.random.uniform(fast_key, (2, HEADS), minval=math.log(1.0 / 50.0), maxval=math.log(1.0 / 17.0)))
    slow_rate = jnp.exp(jax.random.uniform(slow_key, (2, HEADS), minval=math.log(0.3), maxval=math.log(2.0))) / TOKENS
    return jnp.log(jnp.where(fast, fast_rate, slow_rate)).astype(jnp.float32)


def draw_col_order(key, part):
    base = jax.random.fold_in(key, 13)
    perm_key, turn_key = jax.random.split(base, 2)
    columns = jax.random.permutation(perm_key, WIDTH_CELLS).astype(jnp.int32)
    downward = jax.random.randint(turn_key, (WIDTH_CELLS,), 0, 2).astype(jnp.int32)
    position = jnp.arange(TOKENS, dtype=jnp.int32)
    visit = position // FRAME_ROWS
    along = position % FRAME_ROWS
    row_index = jnp.where(downward[visit] == 1, along, FRAME_ROWS - 1 - along)
    return (row_index * WIDTH_CELLS + columns[visit]).astype(jnp.int32)


def steps_of(own_key, shape, shards, least, high):
    factor_of, own = 1.0, jax.random.fold_in(own_key, 6)
    for dim, blocks in shards:
        draws = jnp.exp(jax.random.uniform(jax.random.fold_in(own, dim), (blocks,), jnp.float32, least / len(shards), high / len(shards)))
        factor_of = factor_of * jnp.repeat(draws, shape[dim] // blocks).reshape([-1 if axis == dim else 1 for axis in range(len(shape))])
    return factor_of


def normal_values(key, dims, scale, bound, cuts=(), kind=jnp.bfloat16):
    gain = steps_of(key, dims, cuts, -0.22, 0.18) if cuts else 1.0
    drawn = jax.random.normal(key, dims, jnp.float32) * scale * gain
    return jnp.minimum(jnp.maximum(drawn, -bound), bound).astype(kind)


def setup_inputs(seed: int = 0) -> dict:
    keys = jax.random.split(jax.random.key(seed), 14)
    return {
        "tokens": draw_tokens(jax.random.fold_in(keys[13], 71), 0),
        "col_order": draw_col_order(jax.random.fold_in(keys[13], 71), 0),
        "in_gain": jnp.clip(1.0 + 0.1 * jax.random.normal(keys[2], (2, D), jnp.float32), 0.5, 1.5),
        "w_in": normal_values(keys[3], (2, D, 2, INNER), D ** -0.5, 0.125, ((3, 4),)),
        "w_bc": normal_values(keys[4], (2, D, 2 * STATE), (4 * D) ** -0.5, 0.0625),
        "w_dt": draw_w_dt(jax.random.fold_in(keys[13], 71), 0),
        "conv_x": normal_values(keys[6], (2, CONV, INNER), 0.5, 3.0, ((2, 4),), jnp.float32),
        "conv_bc": normal_values(keys[7], (2, CONV, 2 * STATE), 0.5, 3.0, (), jnp.float32),
        "dt_bias": jnp.clip(-1.0 + 1.5 * jax.random.uniform(keys[8], (2, HEADS), jnp.float32) ** steps_of(keys[8], (2, HEADS), ((1, 4),), -0.2, 0.2), -1.0, 0.5),
        "a_log": draw_a_log(jax.random.fold_in(keys[13], 71), 0),
        "d_skip": jnp.clip(0.5 + 1.5 * jax.random.uniform(keys[10], (2, HEADS), jnp.float32) ** steps_of(keys[10], (2, HEADS), ((1, 4),), -0.2, 0.2), 0.5, 2.0),
        "out_gain": jnp.clip(1.0 + 0.1 * jax.random.normal(keys[11], (2, INNER), jnp.float32), 0.5, 1.5),
        "w_out": normal_values(keys[12], (2, INNER, D), INNER ** -0.5, 0.125, ((1, 4),)),
    }


highest = lax.Precision.HIGHEST
epsilon = 1e-05

def causal_mix(signal, taps):
    length = signal.shape[0]
    padded = jnp.concatenate([jnp.zeros((CONV - 1, signal.shape[1]), jnp.float32), signal.astype(jnp.float32)], axis=0)
    mixed = jnp.zeros((length, signal.shape[1]), jnp.float32)
    for offset in range(CONV):
        mixed = mixed + taps[offset] * padded[offset:offset + length]
    return mixed

def block_step(state, pieces):
    decay_log, b_rows, c_rows, feed = pieces
    cumul = jnp.cumsum(decay_log, axis=0)
    cumul_t = cumul.T
    lower = jnp.arange(STRETCH)[:, None] >= jnp.arange(STRETCH)[None, :]
    spread = jnp.where(lower[None], cumul_t[:, :, None] - cumul_t[:, None, :], -jnp.inf)
    weights = jnp.exp(spread)
    intersection = jnp.dot(c_rows, b_rows.T, precision=highest)
    inside = jnp.einsum('hqk,khp->qhp', intersection[None] * weights, feed, precision=highest)
    carried = jnp.einsum('qn,hpn->qhp', c_rows, state, precision=highest) * jnp.exp(cumul)[:, :, None]
    to_end = jnp.exp(cumul_t[:, -1:] - cumul_t)
    fresh = jnp.einsum('hk,kn,khp->hpn', to_end, b_rows, feed, precision=highest)
    new_state = jnp.exp(cumul[-1])[:, None, None] * state + fresh
    return (new_state, inside + carried)

def mix_layer(stream, which, in_gain, w_in, w_bc, w_dt, conv_x, conv_bc, dt_bias, a_log, d_skip, out_gain, w_out):
    widen = stream.astype(jnp.float32)
    scale = lax.rsqrt(lax.optimization_barrier(jnp.mean(widen * widen, axis=-1, keepdims=True)) + epsilon)
    normed = (widen * scale * in_gain[which]).astype(jnp.bfloat16)
    projected = jnp.dot(normed, w_in[which].reshape(D, 2 * INNER), preferred_element_type=jnp.float32)
    pre_x = projected[:, :INNER].astype(jnp.bfloat16)
    gate_z = projected[:, INNER:].astype(jnp.bfloat16)
    pre_bc = jnp.dot(normed, w_bc[which], preferred_element_type=jnp.float32).astype(jnp.bfloat16)
    dt_raw = jnp.dot(normed, w_dt[which], preferred_element_type=jnp.float32)
    conv_out = jax.nn.silu(causal_mix(pre_x, conv_x[which]))
    bc_out = jax.nn.silu(causal_mix(pre_bc, conv_bc[which]))
    step_size = jax.nn.softplus(dt_raw + dt_bias[which])
    decay_log = -step_size * jnp.exp(a_log[which])
    heads_in = conv_out.reshape(TOKENS, HEADS, HEAD_DIM)
    feed = heads_in * step_size[:, :, None]
    blocks = TOKENS // STRETCH
    pieces = (decay_log.reshape(blocks, STRETCH, HEADS), bc_out[:, :STATE].reshape(blocks, STRETCH, STATE), bc_out[:, STATE:].reshape(blocks, STRETCH, STATE), feed.reshape(blocks, STRETCH, HEADS, HEAD_DIM))
    start_state = jnp.zeros((HEADS, HEAD_DIM, STATE), jnp.float32)
    final_state, outputs = lax.scan(block_step, start_state, pieces)
    ssd = outputs.reshape(TOKENS, HEADS, HEAD_DIM) + d_skip[which][None, :, None] * heads_in
    gated = ssd * jax.nn.silu(gate_z.astype(jnp.float32).reshape(TOKENS, HEADS, HEAD_DIM))
    norm_scale = lax.rsqrt(lax.optimization_barrier(jnp.mean(gated * gated, axis=-1, keepdims=True)) + epsilon)
    mixed_heads = (gated * norm_scale * out_gain[which].reshape(HEADS, HEAD_DIM)).reshape(TOKENS, INNER).astype(jnp.bfloat16)
    group = INNER // N_TP
    total = jnp.zeros((TOKENS, D), jnp.float32)
    for member in range(N_TP):
        partial_sum = jnp.dot(mixed_heads[:, member * group:(member + 1) * group], w_out[which][member * group:(member + 1) * group], preferred_element_type=jnp.float32)
        rounded = lax.optimization_barrier(partial_sum.astype(jnp.bfloat16))
        total = total + rounded.astype(jnp.float32)
    return (widen + total).astype(jnp.bfloat16)

def reference(tokens, col_order, in_gain, w_in, w_bc, w_dt, conv_x, conv_bc, dt_bias, a_log, d_skip, out_gain, w_out):
    params = (in_gain, w_in, w_bc, w_dt, conv_x, conv_bc, dt_bias, a_log, d_skip, out_gain, w_out)
    row_result = mix_layer(tokens, 0, *params)
    column_rows = row_result[col_order.astype(jnp.int32)]
    return mix_layer(column_rows, 1, *params)
```

```python
import functools

import jax
import jax.numpy as jnp
from jax import lax
from jax.experimental import pallas as pl
from jax.experimental.pallas import tpu as pltpu
from jax.sharding import PartitionSpec as P

HEAD_DIM = 64
STATE = 128
STRETCH = 128
LANES = 128
HALO = 16
ROWS = 256

highest = lax.Precision.HIGHEST
epsilon = 1e-05
f32 = jnp.float32
bf16 = jnp.bfloat16


def expander(inner):
    head = lax.broadcasted_iota(jnp.int32, (LANES, inner), 0)
    channel = lax.broadcasted_iota(jnp.int32, (LANES, inner), 1)
    return (head == channel // HEAD_DIM).astype(f32)


def expand(values, spreader):
    return jnp.dot(values, spreader, preferred_element_type=f32, precision=highest)


def scan_kernel(
    full_ref, halo_ref, gain_ref, w_ref, taps_ref, bias_ref, rate_ref, skip_ref,
    y_ref, z_ref, c_ref, cum_ref, end_ref, ext_ref, state_ref, sofar_ref,
):
    i = pl.program_id(0)
    rows = full_ref.shape[0]
    inner = y_ref.shape[1]
    mixed = inner + 2 * STATE
    heads = inner // HEAD_DIM
    spreader = expander(inner)

    def normed(v):
        wide = v.astype(f32)
        scale = lax.rsqrt(jnp.mean(wide * wide, axis=-1, keepdims=True) + epsilon)
        return (wide * scale * gain_ref[...]).astype(bf16)

    @pl.when(i == 0)
    def _():
        before = jnp.dot(normed(halo_ref[...]), w_ref[:, :mixed], preferred_element_type=f32)
        ext_ref[0:8, :] = before[HALO - 8 :, :].astype(bf16).astype(f32)
        state_ref[...] = jnp.zeros_like(state_ref)
        sofar_ref[...] = jnp.zeros_like(sofar_ref)

    projected = jnp.dot(normed(full_ref[...]), w_ref[...], preferred_element_type=f32)
    ext_ref[8 : 8 + rows, :] = projected[:, :mixed].astype(bf16).astype(f32)
    conv = jnp.zeros((rows, mixed), f32)
    count = taps_ref.shape[0]
    for k in range(count):
        conv = conv + taps_ref[k : k + 1, :] * ext_ref[9 - count + k : 9 - count + k + rows, :]
    conv = conv * jax.nn.sigmoid(conv)
    ext_ref[0:8, :] = ext_ref[rows : rows + 8, :]
    z_ref[...] = projected[:, mixed : mixed + inner].astype(bf16)
    raw = projected[:, mixed + inner :] + bias_ref[...]
    step = jnp.maximum(raw, 0.0) + jnp.log1p(jnp.exp(-jnp.abs(raw)))
    logs = -step * rate_ref[...]
    x = conv[:, :inner]
    b_all = conv[:, inner : inner + STATE]
    c_all = conv[:, inner + STATE :].astype(bf16)
    c_ref[...] = c_all
    feed = x * expand(step, spreader)

    row = lax.broadcasted_iota(jnp.int32, (STRETCH, STRETCH), 0)
    col = lax.broadcasted_iota(jnp.int32, (STRETCH, STRETCH), 1)
    lower = row >= col
    tri = lower.astype(f32)
    left = lax.broadcasted_iota(jnp.int32, (STRETCH, 2 * HEAD_DIM), 1) < HEAD_DIM
    state = state_ref[...]
    sofar = sofar_ref[...]
    for block in range(rows // STRETCH):
        part = slice(block * STRETCH, (block + 1) * STRETCH)
        cum = jnp.dot(tri, logs[part], preferred_element_type=f32, precision=highest)
        cum_t = cum.T
        last = cum[STRETCH - 1 : STRETCH, :]
        b_rows = b_all[part]
        c_rows = c_all[part]
        meet = lax.dot_general(
            c_rows, b_rows.astype(bf16), (((1,), (1,)), ((), ())), preferred_element_type=f32
        )
        factors = expand(
            jnp.concatenate([jnp.exp(cum), jnp.exp(last - cum)], axis=0), spreader
        )
        grown = factors[:STRETCH]
        feed_rows = feed[part]
        carried = jnp.dot(c_rows, state.astype(bf16), preferred_element_type=f32) * grown
        fresh = jnp.dot(
            b_rows.T.astype(bf16),
            (feed_rows * factors[STRETCH:]).astype(bf16),
            preferred_element_type=f32,
        )
        state = state * grown[STRETCH - 1 : STRETCH, :] + fresh
        carried = carried + skip_ref[...] * x[part]
        for pair in range(heads // 2):
            lanes = slice(pair * 2 * HEAD_DIM, (pair + 1) * 2 * HEAD_DIM)
            weights = []
            for h in (2 * pair, 2 * pair + 1):
                spread = jnp.where(lower, cum[:, h : h + 1] - cum_t[h : h + 1, :], -jnp.inf)
                weights.append((meet * jnp.exp(spread)).astype(bf16))
            fed = feed_rows[:, lanes]
            stacked = jnp.concatenate(
                [jnp.where(left, fed, 0.0), jnp.where(left, 0.0, fed)], axis=0
            ).astype(bf16)
            inside = jnp.dot(
                jnp.concatenate(weights, axis=1), stacked, preferred_element_type=f32
            )
            y_ref[part, lanes] = inside + carried[:, lanes]
        cum_ref[part, :] = cum + sofar[0:1, :]
        sofar = sofar + last
    state_ref[...] = state
    sofar_ref[...] = sofar

    @pl.when(i == pl.num_programs(0) - 1)
    def _():
        end_ref[0:STATE, :] = state.astype(bf16)
        total = expand(jnp.concatenate([sofar, sofar], axis=0), spreader)
        high = total.astype(bf16)
        rest = total - high.astype(f32)
        middle = rest.astype(bf16)
        low = (rest - middle.astype(f32)).astype(bf16)
        line = lax.broadcasted_iota(jnp.int32, total.shape, 0)
        end_ref[STATE:, :] = jnp.where(
            line == 0,
            high.astype(f32),
            jnp.where(line == 1, middle.astype(f32), low.astype(f32)),
        ).astype(bf16)


def out_kernel(
    y_ref, z_ref, c_ref, cum_ref, ends_ref, gain_ref, w_ref, o_ref, arriving_ref
):
    inner = y_ref.shape[1]
    own = lax.axis_index("seq")

    @pl.when(pl.program_id(0) == 0)
    def _():
        state = jnp.zeros((STATE, inner), f32)
        for m in range(ends_ref.shape[0]):
            tail = ends_ref[m, STATE:, :].astype(f32)
            log = tail[0:1] + tail[1:2] + tail[2:3]
            onward = state * jnp.exp(log) + ends_ref[m, :STATE, :].astype(f32)
            state = jnp.where(m < own, onward, state)
        arriving_ref[...] = state.astype(bf16)

    correction = jnp.dot(c_ref[...], arriving_ref[...], preferred_element_type=f32)
    correction = correction * expand(jnp.exp(cum_ref[...]), expander(inner))
    gate = z_ref[...].astype(f32)
    gated = (y_ref[...] + correction) * (gate * jax.nn.sigmoid(gate))
    pair = 2 * HEAD_DIM
    one = lax.broadcasted_iota(jnp.int32, (2 * pair, pair), 0) % pair // HEAD_DIM
    two = lax.broadcasted_iota(jnp.int32, (2 * pair, pair), 1) // HEAD_DIM
    averager = jnp.where(one == two, 1.0 / HEAD_DIM, 0.0).astype(bf16)
    square = gated * gated
    high = square.astype(bf16)
    low = (square - high.astype(f32)).astype(bf16)
    pieces = []
    for p in range(inner // pair):
        lanes = slice(p * pair, (p + 1) * pair)
        both = jnp.concatenate([high[:, lanes], low[:, lanes]], axis=1)
        mean = jnp.dot(both, averager, preferred_element_type=f32)
        pieces.append(
            (gated[:, lanes] * lax.rsqrt(mean + epsilon) * gain_ref[:, lanes]).astype(bf16)
        )
    mixed_heads = jnp.concatenate(pieces, axis=1)
    o_ref[...] = jnp.dot(mixed_heads, w_ref[...], preferred_element_type=f32).astype(bf16)


def whole(shape):
    return pl.BlockSpec(shape, lambda i: (0,) * len(shape))


def blocked(columns):
    return pl.BlockSpec((ROWS, columns), lambda i: (i, 0))


def mixer(full, halo, params):
    gain, weights, taps, bias, rate, skip, out_gain, w_out = params
    row_count, width = full.shape
    inner = w_out.shape[0]
    mixed = inner + 2 * STATE
    steps = row_count // ROWS
    limit = pltpu.CompilerParams(
        dimension_semantics=("arbitrary",), vmem_limit_bytes=48 * 1024 * 1024
    )
    y, z, c, cum, end = pl.pallas_call(
        scan_kernel,
        grid=(steps,),
        in_specs=[
            blocked(width), whole(halo.shape), whole(gain.shape), whole(weights.shape),
            whole(taps.shape), whole(bias.shape), whole(rate.shape), whole(skip.shape),
        ],
        out_specs=[
            blocked(inner), blocked(inner), blocked(STATE), blocked(LANES),
            whole((STATE + HALO, inner)),
        ],
        out_shape=[
            jax.ShapeDtypeStruct((row_count, inner), f32),
            jax.ShapeDtypeStruct((row_count, inner), bf16),
            jax.ShapeDtypeStruct((row_count, STATE), bf16),
            jax.ShapeDtypeStruct((row_count, LANES), f32),
            jax.ShapeDtypeStruct((STATE + HALO, inner), bf16),
        ],
        scratch_shapes=[
            pltpu.VMEM((ROWS + 8, mixed), f32),
            pltpu.VMEM((STATE, inner), f32),
            pltpu.VMEM((8, LANES), f32),
        ],
        compiler_params=limit,
        cost_estimate=pl.CostEstimate(
            flops=2 * row_count * width * weights.shape[1],
            bytes_accessed=2 * row_count * width + 2 * weights.size,
            transcendentals=0,
        ),
        name="scan_rows",
    )(full, halo, gain, weights, taps, bias, rate, skip)
    ends = lax.all_gather(end, "seq", axis=0)
    return pl.pallas_call(
        out_kernel,
        grid=(steps,),
        in_specs=[
            blocked(inner), blocked(inner), blocked(STATE), blocked(LANES),
            whole(ends.shape), whole(out_gain.shape), whole(w_out.shape),
        ],
        out_specs=blocked(w_out.shape[1]),
        out_shape=jax.ShapeDtypeStruct((row_count, w_out.shape[1]), bf16),
        scratch_shapes=[pltpu.VMEM((STATE, inner), bf16)],
        compiler_params=limit,
        cost_estimate=pl.CostEstimate(
            flops=2 * row_count * inner * w_out.shape[1],
            bytes_accessed=2 * row_count * w_out.shape[1] + 2 * w_out.size,
            transcendentals=0,
        ),
        name="project_out",
    )(y, z, c, cum, ends, out_gain, w_out)


def spread_features(piece):
    return lax.all_gather(piece, "tp", axis=1, tiled=True)


def halo_rows(piece):
    count = lax.axis_size("seq")
    tail = piece[piece.shape[0] - HALO :]
    return spread_features(lax.ppermute(tail, "seq", [(i, i + 1) for i in range(count - 1)]))


def collect_heads(partial_sum):
    return lax.psum_scatter(partial_sum, "tp", scatter_dimension=1, tiled=True).astype(f32)


def ranks(member):
    length = member.shape[-1]
    upto = jnp.arange(length)[:, None] <= jnp.arange(length)[None, :]
    counted = jnp.dot(member.astype(bf16), upto.astype(bf16), preferred_element_type=f32)
    return counted.astype(jnp.int32) - 1


def reorder_plans(col_order):
    count = lax.axis_size("seq")
    own = lax.axis_index("seq")
    length = col_order.shape[0]
    share = length // count
    orders = lax.all_gather(col_order, "seq", axis=0)
    mine = orders // length == own
    rank = ranks(mine)
    slot = jnp.where(mine, rank, -1)
    chosen = slot[:, None, :] == jnp.arange(share)[None, :, None]
    wanted = jnp.sum(jnp.where(chosen, (orders % length)[:, None, :], 0), axis=2).reshape(-1)
    hand = (wanted[:, None] == jnp.arange(length)[None, :]).astype(bf16)
    source = col_order // length
    from_each = source[None, :] == jnp.arange(count)[:, None]
    arrived = jnp.sum(
        jnp.where(from_each, ranks(from_each) + share * jnp.arange(count)[:, None], 0), axis=0
    )
    place = (arrived[:, None] == jnp.arange(length)[None, :]).astype(bf16)
    return hand, place


def pick(plan, rows):
    return jnp.dot(plan, rows, preferred_element_type=f32).astype(bf16)


def reorder_rows(stream, plans):
    hand, place = plans
    arrived = lax.all_to_all(pick(hand, stream), "seq", split_axis=0, concat_axis=0, tiled=True)
    return pick(place, arrived)


def body(
    tokens, col_order, in_gain, w_in, w_bc, w_dt, conv_x, conv_bc,
    dt_bias, a_log, d_skip, out_gain, w_out,
):
    inner = w_in.shape[3]
    pad = LANES - dt_bias.shape[1]

    def layer(which):
        weights = jnp.concatenate(
            [
                w_in[which, :, 0], w_bc[which], w_in[which, :, 1],
                jnp.pad(w_dt[which], ((0, 0), (0, pad))),
            ],
            axis=1,
        )
        return (
            in_gain[which][None],
            weights,
            jnp.concatenate([conv_x[which], conv_bc[which]], axis=1),
            jnp.pad(dt_bias[which], (0, pad))[None],
            jnp.pad(jnp.exp(a_log[which]), (0, pad))[None],
            jnp.repeat(d_skip[which], HEAD_DIM, total_repeat_length=inner)[None],
            out_gain[which][None],
            w_out[which],
        )

    plans = reorder_plans(col_order)
    first = mixer(spread_features(tokens), halo_rows(tokens), layer(0))
    row_result = (tokens.astype(f32) + collect_heads(first)).astype(bf16)
    own_rows = reorder_rows(row_result, plans)
    second = mixer(spread_features(own_rows), halo_rows(own_rows), layer(1))
    return (own_rows.astype(f32) + collect_heads(second)).astype(bf16)


def solution(mesh):
    placed = (
        P("seq", "tp"),
        P("seq"),
        P(),
        P(None, None, None, "tp"),
        P(),
        P(None, None, "tp"),
        P(None, None, "tp"),
        P(),
        P(None, "tp"),
        P(None, "tp"),
        P(None, "tp"),
        P(None, "tp"),
        P(None, "tp", None),
    )
    return jax.shard_map(
        body, mesh=mesh, in_specs=placed, out_specs=P("seq", "tp"), check_vma=False
    )
```

```python
import functools

import jax
import jax.numpy as jnp
from jax import lax
from jax.experimental import pallas as pl
from jax.experimental.pallas import tpu as pltpu
from jax.sharding import PartitionSpec as P

HEAD_DIM = 64
STATE = 128
STRETCH = 128
LANES = 128
HALO = 16
ROWS = 256

highest = lax.Precision.HIGHEST
epsilon = 1e-05
f32 = jnp.float32
bf16 = jnp.bfloat16


def expander(inner):
    head = lax.broadcasted_iota(jnp.int32, (LANES, inner), 0)
    channel = lax.broadcasted_iota(jnp.int32, (LANES, inner), 1)
    return (head == channel // HEAD_DIM).astype(f32)


def expand(values, spreader):
    return jnp.dot(values, spreader, preferred_element_type=f32, precision=highest)


def scan_kernel(
    full_ref, halo_ref, gain_ref, w_ref, taps_ref, bias_ref, rate_ref, skip_ref,
    y_ref, z_ref, c_ref, cum_ref, end_ref, ext_ref, state_ref, sofar_ref,
):
    i = pl.program_id(0)
    rows = full_ref.shape[0]
    inner = y_ref.shape[1]
    mixed = inner + 2 * STATE
    heads = inner // HEAD_DIM
    spreader = expander(inner)

    def normed(v):
        wide = v.astype(f32)
        scale = lax.rsqrt(jnp.mean(wide * wide, axis=-1, keepdims=True) + epsilon)
        return (wide * scale * gain_ref[...]).astype(bf16)

    @pl.when(i == 0)
    def _():
        before = jnp.dot(normed(halo_ref[...]), w_ref[:, :mixed], preferred_element_type=f32)
        ext_ref[0:8, :] = before[HALO - 8 :, :].astype(bf16).astype(f32)
        state_ref[...] = jnp.zeros_like(state_ref)
        sofar_ref[...] = jnp.zeros_like(sofar_ref)

    projected = jnp.dot(normed(full_ref[...]), w_ref[...], preferred_element_type=f32)
    ext_ref[8 : 8 + rows, :] = projected[:, :mixed].astype(bf16).astype(f32)
    conv = jnp.zeros((rows, mixed), f32)
    count = taps_ref.shape[0]
    for k in range(count):
        conv = conv + taps_ref[k : k + 1, :] * ext_ref[9 - count + k : 9 - count + k + rows, :]
    conv = conv * jax.nn.sigmoid(conv)
    ext_ref[0:8, :] = ext_ref[rows : rows + 8, :]
    z_ref[...] = projected[:, mixed : mixed + inner].astype(bf16)
    raw = projected[:, mixed + inner :] + bias_ref[...]
    step = jnp.maximum(raw, 0.0) + jnp.log1p(jnp.exp(-jnp.abs(raw)))
    logs = -step * rate_ref[...]
    x = conv[:, :inner]
    b_all = conv[:, inner : inner + STATE]
    c_all = conv[:, inner + STATE :].astype(bf16)
    c_ref[...] = c_all
    feed = x * expand(step, spreader)

    row = lax.broadcasted_iota(jnp.int32, (STRETCH, STRETCH), 0)
    col = lax.broadcasted_iota(jnp.int32, (STRETCH, STRETCH), 1)
    lower = row >= col
    tri = lower.astype(f32)
    left = lax.broadcasted_iota(jnp.int32, (STRETCH, 2 * HEAD_DIM), 1) < HEAD_DIM
    state = state_ref[...]
    sofar = sofar_ref[...]
    for block in range(rows // STRETCH):
        part = slice(block * STRETCH, (block + 1) * STRETCH)
        cum = jnp.dot(tri, logs[part], preferred_element_type=f32, precision=highest)
        cum_t = cum.T
        last = cum[STRETCH - 1 : STRETCH, :]
        b_rows = b_all[part]
        c_rows = c_all[part]
        meet = lax.dot_general(
            c_rows, b_rows.astype(bf16), (((1,), (1,)), ((), ())), preferred_element_type=f32
        )
        factors = expand(
            jnp.concatenate([jnp.exp(cum), jnp.exp(last - cum)], axis=0), spreader
        )
        grown = factors[:STRETCH]
        feed_rows = feed[part]
        carried = jnp.dot(c_rows, state.astype(bf16), preferred_element_type=f32) * grown
        fresh = jnp.dot(
            b_rows.T.astype(bf16),
            (feed_rows * factors[STRETCH:]).astype(bf16),
            preferred_element_type=f32,
        )
        state = state * grown[STRETCH - 1 : STRETCH, :] + fresh
        carried = carried + skip_ref[...] * x[part]
        for pair in range(heads // 2):
            lanes = slice(pair * 2 * HEAD_DIM, (pair + 1) * 2 * HEAD_DIM)
            weights = []
            for h in (2 * pair, 2 * pair + 1):
                spread = jnp.where(lower, cum[:, h : h + 1] - cum_t[h : h + 1, :], -jnp.inf)
                weights.append((meet * jnp.exp(spread)).astype(bf16))
            fed = feed_rows[:, lanes]
            stacked = jnp.concatenate(
                [jnp.where(left, fed, 0.0), jnp.where(left, 0.0, fed)], axis=0
            ).astype(bf16)
            inside = jnp.dot(
                jnp.concatenate(weights, axis=1), stacked, preferred_element_type=f32
            )
            y_ref[part, lanes] = inside + carried[:, lanes]
        cum_ref[part, :] = cum + sofar[0:1, :]
        sofar = sofar + last
    state_ref[...] = state
    sofar_ref[...] = sofar

    @pl.when(i == pl.num_programs(0) - 1)
    def _():
        end_ref[0:STATE, :] = state.astype(bf16)
        end_ref[STATE:, :] = log_rows(expand(sofar, spreader)[0:1])


def out_kernel(y_ref, z_ref, c_ref, cum_ref, arriving_ref, gain_ref, w_ref, o_ref):
    inner = y_ref.shape[1]
    correction = jnp.dot(c_ref[...], arriving_ref[...], preferred_element_type=f32)
    correction = correction * expand(jnp.exp(cum_ref[...]), expander(inner))
    gate = z_ref[...].astype(f32)
    gated = (y_ref[...] + correction) * (gate * jax.nn.sigmoid(gate))
    pair = 2 * HEAD_DIM
    one = lax.broadcasted_iota(jnp.int32, (2 * pair, pair), 0) % pair // HEAD_DIM
    two = lax.broadcasted_iota(jnp.int32, (2 * pair, pair), 1) // HEAD_DIM
    averager = jnp.where(one == two, 1.0 / HEAD_DIM, 0.0).astype(bf16)
    square = gated * gated
    high = square.astype(bf16)
    low = (square - high.astype(f32)).astype(bf16)
    pieces = []
    for p in range(inner // pair):
        lanes = slice(p * pair, (p + 1) * pair)
        both = jnp.concatenate([high[:, lanes], low[:, lanes]], axis=1)
        mean = jnp.dot(both, averager, preferred_element_type=f32)
        pieces.append(
            (gated[:, lanes] * lax.rsqrt(mean + epsilon) * gain_ref[:, lanes]).astype(bf16)
        )
    mixed_heads = jnp.concatenate(pieces, axis=1)
    o_ref[...] = jnp.dot(mixed_heads, w_ref[...], preferred_element_type=f32).astype(bf16)


def meet_all(partners):
    barrier = pltpu.get_barrier_semaphore()
    for partner in partners:
        pl.semaphore_signal(
            barrier, inc=1, device_id=partner, device_id_type=pl.DeviceIdType.MESH
        )
    pl.semaphore_wait(barrier, len(partners))


def log_of(tail):
    wide = tail.astype(f32)
    return wide[0:1] + wide[1:2] + wide[2:3]


def log_rows(log):
    total = jnp.broadcast_to(log, (HALO, log.shape[1]))
    high = total.astype(bf16).astype(f32)
    middle = (total - high).astype(bf16).astype(f32)
    low = (total - high) - middle
    line = lax.broadcasted_iota(jnp.int32, total.shape, 0)
    return jnp.where(line == 0, high, jnp.where(line == 1, middle, low)).astype(bf16)


def exchange_kernel(
    count, end_ref, arriving_ref, send_ref, got_ref, total_ref, prefix_ref, send_sem, recv_sem
):
    own = lax.axis_index("seq")
    other = lax.axis_index("tp")
    partners, uppers = [], []
    size = 2
    while size <= count:
        place = own % size
        base = own - place
        partner = base + (1 - place if size == 2 else size - 2 - place + 2 * (place % 2))
        partners.append((partner, other))
        uppers.append(place // (size // 2) == 1)
        size *= 2
    meet_all(partners)
    total_ref[...] = end_ref[:STATE, :].astype(f32)
    prefix_ref[...] = jnp.zeros_like(prefix_ref)
    total_log = log_of(end_ref[STATE:, :])
    prefix_log = jnp.zeros_like(total_log)
    for step, (partner, upper) in enumerate(zip(partners, uppers)):
        if step:
            send_ref[step - 1, :STATE, :] = total_ref[...].astype(bf16)
            send_ref[step - 1, STATE:, :] = log_rows(total_log)
        copy = pltpu.make_async_remote_copy(
            src_ref=send_ref.at[step - 1] if step else end_ref,
            dst_ref=got_ref.at[step],
            send_sem=send_sem.at[step],
            recv_sem=recv_sem.at[step],
            device_id=partner,
            device_id_type=pl.DeviceIdType.MESH,
        )
        copy.start()
        copy.wait()
        theirs = got_ref[step, :STATE, :].astype(f32)
        their_log = log_of(got_ref[step, STATE:, :])
        prefix = prefix_ref[...]
        prefix_ref[...] = jnp.where(upper, theirs * jnp.exp(prefix_log) + prefix, prefix)
        prefix_log = jnp.where(upper, prefix_log + their_log, prefix_log)
        if step + 1 < len(partners):
            mine = total_ref[...]
            first = jnp.where(upper, theirs, mine)
            then = jnp.where(upper, mine, theirs)
            total_ref[...] = first * jnp.exp(jnp.where(upper, total_log, their_log)) + then
            total_log = total_log + their_log
    arriving_ref[...] = prefix_ref[...].astype(bf16)


def exchange_states(end):
    count = lax.axis_size("seq")
    steps = count.bit_length() - 1
    inner = end.shape[1]
    vmem = pl.BlockSpec(memory_space=pltpu.VMEM)
    return pl.pallas_call(
        functools.partial(exchange_kernel, count),
        in_specs=[vmem],
        out_specs=vmem,
        out_shape=jax.ShapeDtypeStruct((STATE, inner), bf16),
        scratch_shapes=[
            pltpu.VMEM((max(steps - 1, 1),) + end.shape, bf16),
            pltpu.VMEM((steps,) + end.shape, bf16),
            pltpu.VMEM((STATE, inner), f32),
            pltpu.VMEM((STATE, inner), f32),
            pltpu.SemaphoreType.DMA((steps,)),
            pltpu.SemaphoreType.DMA((steps,)),
        ],
        compiler_params=pltpu.CompilerParams(collective_id=0, has_side_effects=True),
        name="exchange_states",
    )(end)


def collect_kernel(
    partial_ref, stream_ref, out_ref, near_ref, sum_ref, far_ref,
    near_send, near_recv, far_send, far_recv,
):
    seq = lax.axis_index("seq")
    own = lax.axis_index("tp")
    chip, core = own // 2, own % 2
    partner = (seq, chip * 2 + 1 - core)
    across = (seq, (1 - chip) * 2 + core)
    rows, width = out_ref.shape
    chunks = near_send.shape[1]
    size = rows // chunks

    def columns(block):
        return pl.ds(pl.multiple_of(block * width, LANES), width)

    meet_all([partner, across])
    near = []
    for side, block in ((0, (1 - chip) * 2 + 1 - core), (1, chip * 2 + 1 - core)):
        for k in range(chunks):
            part = pl.ds(k * size, size)
            copy = pltpu.make_async_remote_copy(
                src_ref=partial_ref.at[part, columns(block)],
                dst_ref=near_ref.at[side, part],
                send_sem=near_send.at[side, k],
                recv_sem=near_recv.at[side, k],
                device_id=partner,
                device_id_type=pl.DeviceIdType.MESH,
            )
            copy.start()
            near.append(copy)
    far = []
    for k in range(chunks):
        part = pl.ds(k * size, size)
        near[k].wait_recv()
        sum_ref[part, :] = (
            partial_ref[part, columns((1 - chip) * 2 + core)].astype(f32)
            + near_ref[0, part, :].astype(f32)
        ).astype(bf16)
        copy = pltpu.make_async_remote_copy(
            src_ref=sum_ref.at[part],
            dst_ref=far_ref.at[part],
            send_sem=far_send.at[k],
            recv_sem=far_recv.at[k],
            device_id=across,
            device_id_type=pl.DeviceIdType.MESH,
        )
        copy.start()
        far.append(copy)
    for k in range(chunks):
        part = pl.ds(k * size, size)
        near[chunks + k].wait_recv()
        far[k].wait_recv()
        out_ref[part, :] = (
            stream_ref[part, :].astype(f32)
            + partial_ref[part, columns(own)].astype(f32)
            + near_ref[1, part, :].astype(f32)
            + far_ref[part, :].astype(f32)
        ).astype(bf16)
    for copy in near + far:
        copy.wait_send()


def collect_heads(partial_sum, stream):
    rows, width = stream.shape
    chunks = 8
    vmem = pl.BlockSpec(memory_space=pltpu.VMEM)
    return pl.pallas_call(
        collect_kernel,
        in_specs=[vmem, vmem],
        out_specs=vmem,
        out_shape=jax.ShapeDtypeStruct(stream.shape, bf16),
        scratch_shapes=[
            pltpu.VMEM((2, rows, width), bf16),
            pltpu.VMEM((rows, width), bf16),
            pltpu.VMEM((rows, width), bf16),
            pltpu.SemaphoreType.DMA((2, chunks)),
            pltpu.SemaphoreType.DMA((2, chunks)),
            pltpu.SemaphoreType.DMA((chunks,)),
            pltpu.SemaphoreType.DMA((chunks,)),
        ],
        compiler_params=pltpu.CompilerParams(
            collective_id=1, has_side_effects=True, vmem_limit_bytes=40 * 1024 * 1024
        ),
        name="collect_heads",
    )(partial_sum, stream)


def whole(shape):
    return pl.BlockSpec(shape, lambda i: (0,) * len(shape))


def blocked(columns):
    return pl.BlockSpec((ROWS, columns), lambda i: (i, 0))


def mixer(full, halo, params):
    gain, weights, taps, bias, rate, skip, out_gain, w_out = params
    row_count, width = full.shape
    inner = w_out.shape[0]
    mixed = inner + 2 * STATE
    steps = row_count // ROWS
    limit = pltpu.CompilerParams(
        dimension_semantics=("arbitrary",), vmem_limit_bytes=48 * 1024 * 1024
    )
    y, z, c, cum, end = pl.pallas_call(
        scan_kernel,
        grid=(steps,),
        in_specs=[
            blocked(width), whole(halo.shape), whole(gain.shape), whole(weights.shape),
            whole(taps.shape), whole(bias.shape), whole(rate.shape), whole(skip.shape),
        ],
        out_specs=[
            blocked(inner), blocked(inner), blocked(STATE), blocked(LANES),
            whole((STATE + HALO, inner)),
        ],
        out_shape=[
            jax.ShapeDtypeStruct((row_count, inner), f32),
            jax.ShapeDtypeStruct((row_count, inner), bf16),
            jax.ShapeDtypeStruct((row_count, STATE), bf16),
            jax.ShapeDtypeStruct((row_count, LANES), f32),
            jax.ShapeDtypeStruct((STATE + HALO, inner), bf16),
        ],
        scratch_shapes=[
            pltpu.VMEM((ROWS + 8, mixed), f32),
            pltpu.VMEM((STATE, inner), f32),
            pltpu.VMEM((8, LANES), f32),
        ],
        compiler_params=limit,
        cost_estimate=pl.CostEstimate(
            flops=2 * row_count * width * weights.shape[1],
            bytes_accessed=2 * row_count * width + 2 * weights.size,
            transcendentals=0,
        ),
        name="scan_rows",
    )(full, halo, gain, weights, taps, bias, rate, skip)
    arriving = exchange_states(end)
    return pl.pallas_call(
        out_kernel,
        grid=(steps,),
        in_specs=[
            blocked(inner), blocked(inner), blocked(STATE), blocked(LANES),
            whole(arriving.shape), whole(out_gain.shape), whole(w_out.shape),
        ],
        out_specs=blocked(w_out.shape[1]),
        out_shape=jax.ShapeDtypeStruct((row_count, w_out.shape[1]), bf16),
        compiler_params=limit,
        cost_estimate=pl.CostEstimate(
            flops=2 * row_count * inner * w_out.shape[1],
            bytes_accessed=2 * row_count * w_out.shape[1] + 2 * w_out.size,
            transcendentals=0,
        ),
        name="project_out",
    )(y, z, c, cum, arriving, out_gain, w_out)


def spread_features(piece):
    return lax.all_gather(piece, "tp", axis=1, tiled=True)


def halo_rows(piece):
    count = lax.axis_size("seq")
    tail = piece[piece.shape[0] - HALO :]
    return spread_features(lax.ppermute(tail, "seq", [(i, i + 1) for i in range(count - 1)]))


def plan_kernel(source_ref, local_ref, mine_ref, hand_ref, place_ref):
    own = lax.axis_index("seq")
    count, length = source_ref.shape
    share = length // count
    line = lax.broadcasted_iota(jnp.int32, (length, length), 0)
    lane = lax.broadcasted_iota(jnp.int32, (length, length), 1)
    upto = (line <= lane).astype(bf16)
    device = lax.broadcasted_iota(jnp.int32, (count, length), 0)

    def slots(member):
        ones = jnp.where(member, 1.0, 0.0)
        counted = jnp.dot(ones.astype(bf16), upto, preferred_element_type=f32)
        return jnp.where(member, counted.astype(jnp.int32) - 1, -1)

    slot = slots(source_ref[...] == own)
    short = lax.broadcasted_iota(jnp.int32, (share, length), 0)
    wide = lax.broadcasted_iota(jnp.int32, (share, length), 1)
    for d in range(count):
        chosen = slot[d : d + 1, :] == short
        local = jnp.where(chosen, local_ref[d : d + 1, :], 0).astype(f32)
        wanted = jnp.sum(local, axis=1, keepdims=True).astype(jnp.int32)
        hand_ref[d * share : (d + 1) * share, :] = jnp.where(wanted == wide, 1.0, 0.0).astype(bf16)
    from_each = mine_ref[...] == device
    arrived = jnp.where(from_each, slots(from_each) + share * device, 0).astype(f32)
    target = jnp.sum(arrived, axis=0, keepdims=True).astype(jnp.int32)
    place_ref[...] = jnp.where(line == target, 1.0, 0.0).astype(bf16)


def reorder_plans(col_order):
    length = col_order.shape[0]
    orders = lax.all_gather(col_order, "seq", axis=0)
    vmem = pl.BlockSpec(memory_space=pltpu.VMEM)
    plan = jax.ShapeDtypeStruct((length, length), bf16)
    return pl.pallas_call(
        plan_kernel,
        in_specs=[vmem] * 3,
        out_specs=[vmem] * 2,
        out_shape=[plan, plan],
        compiler_params=pltpu.CompilerParams(vmem_limit_bytes=40 * 1024 * 1024),
        name="reorder_plans",
    )(orders // length, orders % length, (col_order // length)[None])


def pick(plan, rows):
    return jnp.dot(plan, rows, preferred_element_type=f32).astype(bf16)


def reorder_rows(stream, plans):
    hand, place = plans
    arrived = lax.all_to_all(pick(hand, stream), "seq", split_axis=0, concat_axis=0, tiled=True)
    return lax.dot_general(
        place, arrived, (((0,), (0,)), ((), ())), preferred_element_type=f32
    ).astype(bf16)


def body(
    tokens, col_order, in_gain, w_in, w_bc, w_dt, conv_x, conv_bc,
    dt_bias, a_log, d_skip, out_gain, w_out,
):
    inner = w_in.shape[3]
    pad = LANES - dt_bias.shape[1]

    def layer(which):
        weights = jnp.concatenate(
            [
                w_in[which, :, 0], w_bc[which], w_in[which, :, 1],
                jnp.pad(w_dt[which], ((0, 0), (0, pad))),
            ],
            axis=1,
        )
        return (
            in_gain[which][None],
            weights,
            jnp.concatenate([conv_x[which], conv_bc[which]], axis=1),
            jnp.pad(dt_bias[which], (0, pad))[None],
            jnp.pad(jnp.exp(a_log[which]), (0, pad))[None],
            jnp.repeat(d_skip[which], HEAD_DIM, total_repeat_length=inner)[None],
            out_gain[which][None],
            w_out[which],
        )

    plans = reorder_plans(col_order)
    layers = [layer(0), layer(1)]
    full = spread_features(tokens)
    full, plans, layers = lax.optimization_barrier((full, plans, layers))
    first = mixer(full, halo_rows(tokens), layers[0])
    row_result = collect_heads(first, tokens)
    own_rows = reorder_rows(row_result, plans)
    second = mixer(spread_features(own_rows), halo_rows(own_rows), layers[1])
    return collect_heads(second, own_rows)


def solution(mesh):
    placed = (
        P("seq", "tp"),
        P("seq"),
        P(),
        P(None, None, None, "tp"),
        P(),
        P(None, None, "tp"),
        P(None, None, "tp"),
        P(),
        P(None, "tp"),
        P(None, "tp"),
        P(None, "tp"),
        P(None, "tp"),
        P(None, "tp", None),
    )
    return jax.shard_map(
        body, mesh=mesh, in_specs=placed, out_specs=P("seq", "tp"), check_vma=False
    )
```

```python
import functools

import jax
import jax.numpy as jnp
from jax import lax
from jax.experimental import pallas as pl
from jax.experimental.pallas import tpu as pltpu
from jax.sharding import PartitionSpec as P

HEAD_DIM = 64
STATE = 128
STRETCH = 128
LANES = 128
HALO = 16
ROWS = 256

highest = lax.Precision.HIGHEST
epsilon = 1e-05
f32 = jnp.float32
bf16 = jnp.bfloat16


def expander(inner):
    head = lax.broadcasted_iota(jnp.int32, (LANES, inner), 0)
    channel = lax.broadcasted_iota(jnp.int32, (LANES, inner), 1)
    return (head == channel // HEAD_DIM).astype(f32)


def expand(values, spreader):
    return jnp.dot(values, spreader, preferred_element_type=f32, precision=highest)


def scan_kernel(
    full_ref, halo_ref, gain_ref, w_ref, taps_ref, bias_ref, rate_ref, skip_ref,
    y_ref, z_ref, c_ref, cum_ref, end_ref, ext_ref, state_ref, sofar_ref,
):
    i = pl.program_id(0)
    rows = full_ref.shape[0]
    inner = y_ref.shape[1]
    mixed = inner + 2 * STATE
    heads = inner // HEAD_DIM
    spreader = expander(inner)

    def normed(v):
        wide = v.astype(f32)
        scale = lax.rsqrt(jnp.mean(wide * wide, axis=-1, keepdims=True) + epsilon)
        return (wide * scale * gain_ref[...]).astype(bf16)

    @pl.when(i == 0)
    def _():
        before = jnp.dot(normed(halo_ref[...]), w_ref[:, :mixed], preferred_element_type=f32)
        ext_ref[0:8, :] = before[HALO - 8 :, :].astype(bf16).astype(f32)
        state_ref[...] = jnp.zeros_like(state_ref)
        sofar_ref[...] = jnp.zeros_like(sofar_ref)

    projected = jnp.dot(normed(full_ref[...]), w_ref[...], preferred_element_type=f32)
    ext_ref[8 : 8 + rows, :] = projected[:, :mixed].astype(bf16).astype(f32)
    conv = jnp.zeros((rows, mixed), f32)
    count = taps_ref.shape[0]
    for k in range(count):
        conv = conv + taps_ref[k : k + 1, :] * ext_ref[9 - count + k : 9 - count + k + rows, :]
    conv = conv * jax.nn.sigmoid(conv)
    ext_ref[0:8, :] = ext_ref[rows : rows + 8, :]
    z_ref[...] = projected[:, mixed : mixed + inner].astype(bf16)
    raw = projected[:, mixed + inner :] + bias_ref[...]
    step = jnp.maximum(raw, 0.0) + jnp.log1p(jnp.exp(-jnp.abs(raw)))
    logs = -step * rate_ref[...]
    x = conv[:, :inner]
    b_all = conv[:, inner : inner + STATE]
    c_all = conv[:, inner + STATE :].astype(bf16)
    c_ref[...] = c_all
    feed = x * expand(step, spreader)

    row = lax.broadcasted_iota(jnp.int32, (STRETCH, STRETCH), 0)
    col = lax.broadcasted_iota(jnp.int32, (STRETCH, STRETCH), 1)
    lower = row >= col
    tri = lower.astype(f32)
    left = lax.broadcasted_iota(jnp.int32, (STRETCH, 2 * HEAD_DIM), 1) < HEAD_DIM
    skip = expand(jnp.broadcast_to(skip_ref[...], (8, LANES)), spreader)[0:1]
    state = state_ref[...]
    sofar = sofar_ref[...]
    for block in range(rows // STRETCH):
        part = slice(block * STRETCH, (block + 1) * STRETCH)
        cum = jnp.dot(tri, logs[part], preferred_element_type=f32, precision=highest)
        cum_t = cum.T
        last = cum[STRETCH - 1 : STRETCH, :]
        b_rows = b_all[part]
        c_rows = c_all[part]
        meet = lax.dot_general(
            c_rows, b_rows.astype(bf16), (((1,), (1,)), ((), ())), preferred_element_type=f32
        )
        factors = expand(
            jnp.concatenate([jnp.exp(cum), jnp.exp(last - cum)], axis=0), spreader
        )
        grown = factors[:STRETCH]
        feed_rows = feed[part]
        carried = jnp.dot(c_rows, state.astype(bf16), preferred_element_type=f32) * grown
        fresh = jnp.dot(
            b_rows.T.astype(bf16),
            (feed_rows * factors[STRETCH:]).astype(bf16),
            preferred_element_type=f32,
        )
        state = state * grown[STRETCH - 1 : STRETCH, :] + fresh
        carried = carried + skip * x[part]
        for pair in range(heads // 2):
            lanes = slice(pair * 2 * HEAD_DIM, (pair + 1) * 2 * HEAD_DIM)
            weights = []
            for h in (2 * pair, 2 * pair + 1):
                spread = jnp.where(lower, cum[:, h : h + 1] - cum_t[h : h + 1, :], -jnp.inf)
                weights.append((meet * jnp.exp(spread)).astype(bf16))
            fed = feed_rows[:, lanes]
            stacked = jnp.concatenate(
                [jnp.where(left, fed, 0.0), jnp.where(left, 0.0, fed)], axis=0
            ).astype(bf16)
            inside = jnp.dot(
                jnp.concatenate(weights, axis=1), stacked, preferred_element_type=f32
            )
            y_ref[part, lanes] = inside + carried[:, lanes]
        cum_ref[part, :] = cum + sofar[0:1, :]
        sofar = sofar + last
    state_ref[...] = state
    sofar_ref[...] = sofar

    @pl.when(i == pl.num_programs(0) - 1)
    def _():
        end_ref[0:STATE, :] = state.astype(bf16)
        end_ref[STATE:, :] = log_rows(expand(sofar, spreader)[0:1])


def out_kernel(y_ref, z_ref, c_ref, cum_ref, arriving_ref, gain_ref, w_ref, o_ref):
    inner = y_ref.shape[1]
    correction = jnp.dot(c_ref[...], arriving_ref[...], preferred_element_type=f32)
    correction = correction * expand(jnp.exp(cum_ref[...]), expander(inner))
    gate = z_ref[...].astype(f32)
    gated = (y_ref[...] + correction) * (gate * jax.nn.sigmoid(gate))
    pair = 2 * HEAD_DIM
    one = lax.broadcasted_iota(jnp.int32, (2 * pair, pair), 0) % pair // HEAD_DIM
    two = lax.broadcasted_iota(jnp.int32, (2 * pair, pair), 1) // HEAD_DIM
    averager = jnp.where(one == two, 1.0 / HEAD_DIM, 0.0).astype(bf16)
    square = gated * gated
    high = square.astype(bf16)
    low = (square - high.astype(f32)).astype(bf16)
    pieces = []
    for p in range(inner // pair):
        lanes = slice(p * pair, (p + 1) * pair)
        both = jnp.concatenate([high[:, lanes], low[:, lanes]], axis=1)
        mean = jnp.dot(both, averager, preferred_element_type=f32)
        pieces.append(
            (gated[:, lanes] * lax.rsqrt(mean + epsilon) * gain_ref[:, lanes]).astype(bf16)
        )
    mixed_heads = jnp.concatenate(pieces, axis=1)
    o_ref[...] = jnp.dot(mixed_heads, w_ref[...], preferred_element_type=f32).astype(bf16)


def meet_all(partners):
    barrier = pltpu.get_barrier_semaphore()
    for partner in partners:
        pl.semaphore_signal(
            barrier, inc=1, device_id=partner, device_id_type=pl.DeviceIdType.MESH
        )
    pl.semaphore_wait(barrier, len(partners))


def log_of(tail):
    wide = tail.astype(f32)
    return wide[0:1] + wide[1:2] + wide[2:3]


def log_rows(log):
    total = jnp.broadcast_to(log, (HALO, log.shape[1]))
    high = total.astype(bf16).astype(f32)
    middle = (total - high).astype(bf16).astype(f32)
    low = (total - high) - middle
    line = lax.broadcasted_iota(jnp.int32, total.shape, 0)
    return jnp.where(line == 0, high, jnp.where(line == 1, middle, low)).astype(bf16)


def exchange_kernel(
    count, end_ref, arriving_ref, send_ref, got_ref, total_ref, prefix_ref, send_sem, recv_sem
):
    own = lax.axis_index("seq")
    other = lax.axis_index("tp")
    partners, uppers = [], []
    size = 2
    while size <= count:
        place = own % size
        base = own - place
        partner = base + (1 - place if size == 2 else size - 2 - place + 2 * (place % 2))
        partners.append((partner, other))
        uppers.append(place // (size // 2) == 1)
        size *= 2
    meet_all(partners)
    total_ref[...] = end_ref[:STATE, :].astype(f32)
    prefix_ref[...] = jnp.zeros_like(prefix_ref)
    total_log = log_of(end_ref[STATE:, :])
    prefix_log = jnp.zeros_like(total_log)
    for step, (partner, upper) in enumerate(zip(partners, uppers)):
        if step:
            send_ref[step - 1, :STATE, :] = total_ref[...].astype(bf16)
            send_ref[step - 1, STATE:, :] = log_rows(total_log)
        copy = pltpu.make_async_remote_copy(
            src_ref=send_ref.at[step - 1] if step else end_ref,
            dst_ref=got_ref.at[step],
            send_sem=send_sem.at[step],
            recv_sem=recv_sem.at[step],
            device_id=partner,
            device_id_type=pl.DeviceIdType.MESH,
        )
        copy.start()
        copy.wait()
        theirs = got_ref[step, :STATE, :].astype(f32)
        their_log = log_of(got_ref[step, STATE:, :])
        prefix = prefix_ref[...]
        prefix_ref[...] = jnp.where(upper, theirs * jnp.exp(prefix_log) + prefix, prefix)
        prefix_log = jnp.where(upper, prefix_log + their_log, prefix_log)
        if step + 1 < len(partners):
            mine = total_ref[...]
            first = jnp.where(upper, theirs, mine)
            then = jnp.where(upper, mine, theirs)
            total_ref[...] = first * jnp.exp(jnp.where(upper, total_log, their_log)) + then
            total_log = total_log + their_log
    arriving_ref[...] = prefix_ref[...].astype(bf16)


def exchange_states(end):
    count = lax.axis_size("seq")
    steps = count.bit_length() - 1
    inner = end.shape[1]
    vmem = pl.BlockSpec(memory_space=pltpu.VMEM)
    return pl.pallas_call(
        functools.partial(exchange_kernel, count),
        in_specs=[vmem],
        out_specs=vmem,
        out_shape=jax.ShapeDtypeStruct((STATE, inner), bf16),
        scratch_shapes=[
            pltpu.VMEM((max(steps - 1, 1),) + end.shape, bf16),
            pltpu.VMEM((steps,) + end.shape, bf16),
            pltpu.VMEM((STATE, inner), f32),
            pltpu.VMEM((STATE, inner), f32),
            pltpu.SemaphoreType.DMA((steps,)),
            pltpu.SemaphoreType.DMA((steps,)),
        ],
        compiler_params=pltpu.CompilerParams(collective_id=0, has_side_effects=True),
        name="exchange_states",
    )(end)


def collect_kernel(
    partial_ref, stream_ref, out_ref, near_ref, sum_ref, far_ref,
    near_send, near_recv, far_send, far_recv,
):
    seq = lax.axis_index("seq")
    own = lax.axis_index("tp")
    chip, core = own // 2, own % 2
    partner = (seq, chip * 2 + 1 - core)
    across = (seq, (1 - chip) * 2 + core)
    rows, width = out_ref.shape
    chunks = near_send.shape[1]
    size = rows // chunks

    def columns(block):
        return pl.ds(pl.multiple_of(block * width, LANES), width)

    meet_all([partner, across])
    near = []
    for side, block in ((0, (1 - chip) * 2 + 1 - core), (1, chip * 2 + 1 - core)):
        for k in range(chunks):
            part = pl.ds(k * size, size)
            copy = pltpu.make_async_remote_copy(
                src_ref=partial_ref.at[part, columns(block)],
                dst_ref=near_ref.at[side, part],
                send_sem=near_send.at[side, k],
                recv_sem=near_recv.at[side, k],
                device_id=partner,
                device_id_type=pl.DeviceIdType.MESH,
            )
            copy.start()
            near.append(copy)
    far = []
    for k in range(chunks):
        part = pl.ds(k * size, size)
        near[k].wait_recv()
        sum_ref[part, :] = (
            partial_ref[part, columns((1 - chip) * 2 + core)].astype(f32)
            + near_ref[0, part, :].astype(f32)
        ).astype(bf16)
        copy = pltpu.make_async_remote_copy(
            src_ref=sum_ref.at[part],
            dst_ref=far_ref.at[part],
            send_sem=far_send.at[k],
            recv_sem=far_recv.at[k],
            device_id=across,
            device_id_type=pl.DeviceIdType.MESH,
        )
        copy.start()
        far.append(copy)
    for k in range(chunks):
        part = pl.ds(k * size, size)
        near[chunks + k].wait_recv()
        far[k].wait_recv()
        out_ref[part, :] = (
            stream_ref[part, :].astype(f32)
            + partial_ref[part, columns(own)].astype(f32)
            + near_ref[1, part, :].astype(f32)
            + far_ref[part, :].astype(f32)
        ).astype(bf16)
    for copy in near + far:
        copy.wait_send()


def collect_heads(partial_sum, stream):
    rows, width = stream.shape
    chunks = 8
    vmem = pl.BlockSpec(memory_space=pltpu.VMEM)
    return pl.pallas_call(
        collect_kernel,
        in_specs=[vmem, vmem],
        out_specs=vmem,
        out_shape=jax.ShapeDtypeStruct(stream.shape, bf16),
        scratch_shapes=[
            pltpu.VMEM((2, rows, width), bf16),
            pltpu.VMEM((rows, width), bf16),
            pltpu.VMEM((rows, width), bf16),
            pltpu.SemaphoreType.DMA((2, chunks)),
            pltpu.SemaphoreType.DMA((2, chunks)),
            pltpu.SemaphoreType.DMA((chunks,)),
            pltpu.SemaphoreType.DMA((chunks,)),
        ],
        compiler_params=pltpu.CompilerParams(
            collective_id=1, has_side_effects=True, vmem_limit_bytes=40 * 1024 * 1024
        ),
        name="collect_heads",
    )(partial_sum, stream)


def whole(shape):
    return pl.BlockSpec(shape, lambda i: (0,) * len(shape))


def blocked(columns):
    return pl.BlockSpec((ROWS, columns), lambda i: (i, 0))


def mixer(full, halo, params):
    gain, weights, taps, bias, rate, skip, out_gain, w_out = params
    row_count, width = full.shape
    inner = w_out.shape[0]
    mixed = inner + 2 * STATE
    steps = row_count // ROWS
    limit = pltpu.CompilerParams(
        dimension_semantics=("arbitrary",), vmem_limit_bytes=48 * 1024 * 1024
    )
    y, z, c, cum, end = pl.pallas_call(
        scan_kernel,
        grid=(steps,),
        in_specs=[
            blocked(width), whole(halo.shape), whole(gain.shape), whole(weights.shape),
            whole(taps.shape), whole(bias.shape), whole(rate.shape), whole(skip.shape),
        ],
        out_specs=[
            blocked(inner), blocked(inner), blocked(STATE), blocked(LANES),
            whole((STATE + HALO, inner)),
        ],
        out_shape=[
            jax.ShapeDtypeStruct((row_count, inner), f32),
            jax.ShapeDtypeStruct((row_count, inner), bf16),
            jax.ShapeDtypeStruct((row_count, STATE), bf16),
            jax.ShapeDtypeStruct((row_count, LANES), f32),
            jax.ShapeDtypeStruct((STATE + HALO, inner), bf16),
        ],
        scratch_shapes=[
            pltpu.VMEM((ROWS + 8, mixed), f32),
            pltpu.VMEM((STATE, inner), f32),
            pltpu.VMEM((8, LANES), f32),
        ],
        compiler_params=limit,
        cost_estimate=pl.CostEstimate(
            flops=2 * row_count * width * weights.shape[1],
            bytes_accessed=2 * row_count * width + 2 * weights.size,
            transcendentals=0,
        ),
        name="scan_rows",
    )(full, halo, gain, weights, taps, bias, rate, skip)
    arriving = exchange_states(end)
    return pl.pallas_call(
        out_kernel,
        grid=(steps,),
        in_specs=[
            blocked(inner), blocked(inner), blocked(STATE), blocked(LANES),
            whole(arriving.shape), whole(out_gain.shape), whole(w_out.shape),
        ],
        out_specs=blocked(w_out.shape[1]),
        out_shape=jax.ShapeDtypeStruct((row_count, w_out.shape[1]), bf16),
        compiler_params=limit,
        cost_estimate=pl.CostEstimate(
            flops=2 * row_count * inner * w_out.shape[1],
            bytes_accessed=2 * row_count * w_out.shape[1] + 2 * w_out.size,
            transcendentals=0,
        ),
        name="project_out",
    )(y, z, c, cum, arriving, out_gain, w_out)


def spread_features(piece):
    return lax.all_gather(piece, "tp", axis=1, tiled=True)


def halo_rows(piece):
    count = lax.axis_size("seq")
    tail = piece[piece.shape[0] - HALO :]
    return spread_features(lax.ppermute(tail, "seq", [(i, i + 1) for i in range(count - 1)]))


def plan_kernel(source_ref, local_ref, mine_ref, hand_ref, place_ref):
    own = lax.axis_index("seq")
    count, length = source_ref.shape
    share = length // count
    line = lax.broadcasted_iota(jnp.int32, (length, length), 0)
    lane = lax.broadcasted_iota(jnp.int32, (length, length), 1)
    upto = (line <= lane).astype(bf16)
    device = lax.broadcasted_iota(jnp.int32, (count, length), 0)

    def slots(member):
        ones = jnp.where(member, 1.0, 0.0)
        counted = jnp.dot(ones.astype(bf16), upto, preferred_element_type=f32)
        return jnp.where(member, counted.astype(jnp.int32) - 1, -1)

    slot = slots(source_ref[...] == own)
    short = lax.broadcasted_iota(jnp.int32, (share, length), 0)
    wide = lax.broadcasted_iota(jnp.int32, (share, length), 1)
    for d in range(count):
        chosen = slot[d : d + 1, :] == short
        local = jnp.where(chosen, local_ref[d : d + 1, :], 0).astype(f32)
        wanted = jnp.sum(local, axis=1, keepdims=True).astype(jnp.int32)
        hand_ref[d * share : (d + 1) * share, :] = jnp.where(wanted == wide, 1.0, 0.0).astype(bf16)
    from_each = mine_ref[...] == device
    arrived = jnp.where(from_each, slots(from_each) + share * device, 0).astype(f32)
    target = jnp.sum(arrived, axis=0, keepdims=True).astype(jnp.int32)
    place_ref[...] = jnp.where(line == target, 1.0, 0.0).astype(bf16)


def reorder_plans(col_order, orders):
    length = col_order.shape[0]
    vmem = pl.BlockSpec(memory_space=pltpu.VMEM)
    plan = jax.ShapeDtypeStruct((length, length), bf16)
    return pl.pallas_call(
        plan_kernel,
        in_specs=[vmem] * 3,
        out_specs=[vmem] * 2,
        out_shape=[plan, plan],
        compiler_params=pltpu.CompilerParams(vmem_limit_bytes=40 * 1024 * 1024),
        name="reorder_plans",
    )(orders // length, orders % length, (col_order // length)[None])


def pick(plan, rows):
    return jnp.dot(plan, rows, preferred_element_type=f32).astype(bf16)


def reorder_rows(stream, plans):
    hand, place = plans
    arrived = lax.all_to_all(pick(hand, stream), "seq", split_axis=0, concat_axis=0, tiled=True)
    return lax.dot_general(
        place, arrived, (((0,), (0,)), ((), ())), preferred_element_type=f32
    ).astype(bf16)


def body(
    tokens, col_order, in_gain, w_in, w_bc, w_dt, conv_x, conv_bc,
    dt_bias, a_log, d_skip, out_gain, w_out,
):
    pad = LANES - dt_bias.shape[1]

    def layer(which):
        weights = jnp.concatenate(
            [
                w_in[which, :, 0], w_bc[which], w_in[which, :, 1],
                jnp.pad(w_dt[which], ((0, 0), (0, pad))),
            ],
            axis=1,
        )
        return (
            in_gain[which][None],
            weights,
            jnp.concatenate([conv_x[which], conv_bc[which]], axis=1),
            jnp.pad(dt_bias[which], (0, pad))[None],
            jnp.pad(jnp.exp(a_log[which]), (0, pad))[None],
            jnp.pad(d_skip[which], (0, pad))[None],
            out_gain[which][None],
            w_out[which],
        )

    orders = lax.all_gather(col_order, "seq", axis=0)
    tokens, orders = lax.optimization_barrier((tokens, orders))
    plans = reorder_plans(col_order, orders)
    layers = [layer(0), layer(1)]
    full = spread_features(tokens)
    full, plans, layers = lax.optimization_barrier((full, plans, layers))
    first = mixer(full, halo_rows(tokens), layers[0])
    row_result = collect_heads(first, tokens)
    own_rows = reorder_rows(row_result, plans)
    second = mixer(spread_features(own_rows), halo_rows(own_rows), layers[1])
    return collect_heads(second, own_rows)


def solution(mesh):
    placed = (
        P("seq", "tp"),
        P("seq"),
        P(),
        P(None, None, None, "tp"),
        P(),
        P(None, None, "tp"),
        P(None, None, "tp"),
        P(),
        P(None, "tp"),
        P(None, "tp"),
        P(None, "tp"),
        P(None, "tp"),
        P(None, "tp", None),
    )
    return jax.shard_map(
        body, mesh=mesh, in_specs=placed, out_specs=P("seq", "tp"), check_vma=False
    )
```
